32 devices in a mesh: band: 8 (over z, core), grid: 4 (over y, x).
Axes of the slice: x: 2, y: 2, z: 4, core: 2. Of those that a mesh axis runs over, the one named last changes fastest.
Arguments:
- orbitals: float32 [8, 48, 2304], P('band', 'grid'), may hold values from -6 to 6
Outputs:
- compressed: float32 [8, 48, 2304], P('band', 'grid')
The draws below stay inside these ranges and needn't reach their ends.
All inputs are finite; a program needn't handle non-finite values.
Results may differ from the reference program's by a relative error of at most 0.000092.
Values sent between devices are 32-bit elements; how exact they have to be, the bound alone decides.
A program may use at most 64 MiB of HBM per device.

```python
import jax
import jax.numpy as jnp
from jax import lax

NG = 48
BANDS = 8


def shard_levels(own_key, shape, pieces, least, top_value):
    level = 1.0
    for dim, blocks in pieces:
        steps = jax.random.uniform(jax.random.fold_in(jax.random.fold_in(own_key, 6), dim), (blocks,), jnp.float32, least / len(pieces), top_value / len(pieces))
        level = level * jnp.repeat(jnp.exp(steps), shape[dim] // blocks).reshape((-1,) + (1,) * (len(shape) - 1 - dim))
    return level


def centred(stream_key, shape, scale, limit, pieces=(), held_as=jnp.bfloat16):
    array = jax.random.normal(stream_key, shape, jnp.float32) * scale
    if len(pieces) > 0:
        array = shard_levels(stream_key, shape, pieces, -0.22, 0.18) * array
    return jnp.clip(array, min=-limit, max=limit).astype(held_as)


def setup_inputs(seed: int = 0) -> dict:
    seeds = jax.random.split(jax.random.key(seed), 2)
    orbitals = centred(seeds[0], (BANDS, NG, NG * NG), 1.0, 6.0, ((0, 8), (1, 4)), jnp.float32)
    return {"orbitals": orbitals}


coulomb_scale = 50.0

def coulomb_table(length):
    counter = jnp.arange(length, dtype=jnp.int32)
    signed = jnp.where(counter < length // 2, counter, counter - length).astype(jnp.float32)
    squares = signed * signed
    summed = squares[:, None, None] + squares[None, :, None] + squares[None, None, :]
    return jnp.where(summed > 0.0, coulomb_scale / jnp.maximum(summed, 1.0), 0.0)

def reference(orbitals):
    band_count = orbitals.shape[0]
    length = orbitals.shape[1]
    fields = orbitals.reshape(band_count, length, length, length)
    kernel = coulomb_table(length)

    def apply_one(orbital):
        density = orbital[None] * fields
        spectrum = jnp.fft.fftn(density, axes=(1, 2, 3))
        potential = jnp.real(jnp.fft.ifftn(spectrum * kernel, axes=(1, 2, 3)))
        return -jnp.sum(fields * potential, axis=0)
    exchange = lax.map(apply_one, fields)
    flat_orbitals = fields.reshape(band_count, -1)
    flat_exchange = exchange.reshape(band_count, -1)
    cells_total = float(length ** 3)
    projected = jnp.dot(flat_orbitals.astype(jnp.float32), flat_exchange.T.astype(jnp.float32), precision=lax.Precision.HIGHEST, preferred_element_type=jnp.float32) / cells_total
    definite = -0.5 * (projected + projected.T)
    lower = jnp.linalg.cholesky(definite)
    inverse_lower = jax.scipy.linalg.solve_triangular(lower, jnp.eye(band_count, dtype=jnp.float32), lower=True)
    compressed = jnp.dot(inverse_lower.astype(jnp.float32), flat_exchange.astype(jnp.float32), precision=lax.Precision.HIGHEST, preferred_element_type=jnp.float32)
    return compressed.reshape(orbitals.shape)
```

```python
import functools
import math

import jax
import jax.numpy as jnp
import numpy as np
from jax import lax
from jax.experimental import pallas as pl
from jax.experimental.pallas import tpu as pltpu
from jax.sharding import PartitionSpec as P

MESH = pl.DeviceIdType.MESH
F32 = jnp.float32
BF16 = jnp.bfloat16
coulomb_scale = 50.0


def real_basis(length):
    n = np.arange(length)[:, None]
    m = np.arange(length)[None, :]
    angle = 2.0 * math.pi * ((n * np.minimum(m, length - m)) % length) / length
    table = np.where(m <= length // 2, np.cos(angle), np.sin(angle))
    weight = np.where((m == 0) | (2 * m == length), 1.0, 2.0)
    return table * np.sqrt(weight / length)


def split(value):
    high = value.astype(BF16)
    return high, (value - high.astype(F32)).astype(BF16)


def times(value, high, low, contract=((1,), (0,))):
    dims = (contract, ((), ()))
    value_high, value_low = split(value)
    dot = functools.partial(lax.dot_general, dimension_numbers=dims, preferred_element_type=F32)
    return dot(value_high, high) + (dot(value_low, high) + dot(value_high, low))


def times_left(high, low, value):
    dims = (((1,), (1,)), ((), ()))
    value_high, value_low = split(value)
    dot = functools.partial(lax.dot_general, dimension_numbers=dims, preferred_element_type=F32)
    return dot(high, value_high) + (dot(high, value_low) + dot(low, value_high))


def flat(value):
    return value.reshape(value.shape[0] * value.shape[1], value.shape[2])


def kernel(
    bands, grids, length,
    phi, tables, out,
    slabs, own, part, field, sums, exs, proj_grid, proj_band,
    dense_own, dense_part, work, coulomb, dense_field, column,
    sem_local, slab_send, slab_recv, fwd_send,
    own_send, own_recv, part_send, part_recv, pfwd_send, pfwd_recv,
    sum_send, sum_recv, ex_send, ex_recv, xfwd_send,
    pg_send, pg_recv, pb_send, pb_recv,
):
    b = lax.axis_index("band")
    g = lax.axis_index("grid")
    p = b // 2
    c = b % 2
    sibling = p * 2 + (1 - c)
    rows = length // grids
    pairs = bands // 2
    step = 8
    chunk = step * length

    def remote(src, dst, send, recv, band, grid):
        return pltpu.make_async_remote_copy(
            src_ref=src, dst_ref=dst, send_sem=send, recv_sem=recv,
            device_id=(band, grid), device_id_type=MESH,
        )

    local = pltpu.make_async_copy(phi, slabs.at[b], sem_local)
    local.start()

    barrier = pltpu.get_barrier_semaphore()
    for off in range(1, bands):
        pl.semaphore_signal(barrier, inc=1, device_id=(lax.rem(b + off, bands), g), device_id_type=MESH)
    for off in range(1, grids):
        pl.semaphore_signal(barrier, inc=1, device_id=(b, lax.rem(g + off, grids)), device_id_type=MESH)
    pl.semaphore_wait(barrier, bands + grids - 2)

    waits = []

    def go(copy):
        copy.start()
        waits.append(copy)

    for off in range(1, pairs):
        peer = lax.rem(p + off, pairs) * 2 + c
        go(remote(phi, slabs.at[b], slab_send.at[off], slab_recv.at[b], peer, g))
    for off in range(1, grids):
        go(remote(phi, own.at[g], own_send.at[off], own_recv.at[g], b, lax.rem(g + off, grids)))
    go(remote(phi, slabs.at[b], slab_send.at[0], slab_recv.at[b], sibling, g))

    def freq(shape, dim, base):
        m = lax.broadcasted_iota(jnp.int32, shape, dim) + base
        f = jnp.minimum(m, length - m).astype(F32)
        return f * f

    def coulomb_step(i, carry):
        shape = (step, length, length)
        squared = freq(shape, 0, i * step) + freq(shape, 1, 0) + freq(shape, 2, 0)
        coulomb[pl.ds(i * step, step)] = jnp.where(
            squared > 0.0, coulomb_scale / jnp.maximum(squared, 1.0), 0.0
        )
        return carry

    lax.fori_loop(0, length // step, coulomb_step, 0)
    local.wait()

    def to_partner(pair):
        copy = remote(
            slabs.at[pair * 2 + c], part.at[c, g], part_send.at[pair], part_recv.at[g], b, pair
        )

        @pl.when(pair != g)
        def _():
            copy.start()

    to_partner(p)
    for off in range(1, pairs):
        pair = lax.rem(p + off, pairs)
        band = pair * 2 + c
        remote(phi, slabs.at[band], slab_send.at[0], slab_recv.at[band], sibling, g).wait_recv()
        to_partner(pair)
        go(remote(slabs.at[band], slabs.at[band], fwd_send.at[off], slab_recv.at[band], sibling, g))

    for off in range(1, grids):
        other = lax.rem(g + off, grids)
        remote(phi, part.at[c, other], part_send.at[0], part_recv.at[other], b, other).wait_recv()
        go(remote(part.at[c, other], part.at[c, other], pfwd_send.at[off], pfwd_recv.at[other], sibling, g))

    for off in range(1, grids):
        other = lax.rem(g + off, grids)
        remote(phi, own.at[other], own_send.at[0], own_recv.at[other], b, other).wait_recv()
    own[g] = phi[...]
    for off in range(pairs):
        band = lax.rem(p + off, pairs) * 2 + (1 - c)
        remote(phi, slabs.at[band], slab_send.at[0], slab_recv.at[band], sibling, g).wait_recv()
    for k in range(2):
        part[k, g] = slabs[2 * g + k]
    for off in range(1, grids):
        other = lax.rem(g + off, grids)
        remote(phi, part.at[1 - c, other], part_send.at[0], pfwd_recv.at[other], sibling, g).wait_recv()

    for s in range(grids):
        dense_own[s * rows:(s + 1) * rows, :] = own[s]
        for k in range(2):
            dense_part[k, s * rows:(s + 1) * rows, :] = part[k, s]

    q_high, q_low, t_high, t_low = (tables[n] for n in range(4))

    def swap(value):
        return jnp.swapaxes(value, 1, 2)

    def unflat(value):
        return value.reshape(value.shape[0] // length, length, length)

    def one_pair(k, carry):
        def stage_in(i, carry):
            lanes = pl.ds(pl.multiple_of(i * chunk, 128), chunk)
            density = dense_own[:, lanes] * dense_part[k, :, lanes]
            first = unflat(times(density.T, q_high, q_low))
            second = unflat(times(flat(swap(first)), q_high, q_low))
            work[pl.ds(i * step, step)] = second
            return carry

        def stage_mid(i, carry):
            here = pl.ds(pl.multiple_of(i * step, step), step)
            value = jnp.swapaxes(work[:, here, :], 0, 1)
            value = unflat(times(flat(swap(value)), q_high, q_low))
            value = value * coulomb[pl.ds(i * step, step)]
            value = unflat(times(flat(value), t_high, t_low))
            work[:, here, :] = jnp.swapaxes(swap(value), 0, 1)
            return carry

        def stage_out(i, carry):
            lanes = pl.ds(pl.multiple_of(i * chunk, 128), chunk)
            value = unflat(times(flat(work[pl.ds(i * step, step)]), t_high, t_low))
            potential = times_left(q_high, q_low, flat(swap(value)))
            term = dense_part[k, :, lanes] * potential

            @pl.when(k == 0)
            def _():
                dense_field[:, lanes] = term

            @pl.when(k != 0)
            def _():
                dense_field[:, lanes] += term

            return carry

        lax.fori_loop(0, length // step, stage_in, 0)
        lax.fori_loop(0, length // step, stage_mid, 0)
        lax.fori_loop(0, length // step, stage_out, 0)
        return carry

    lax.fori_loop(0, 2, one_pair, 0)

    for s in range(grids):
        field[s] = dense_field[s * rows:(s + 1) * rows, :]
    for off in range(1, grids):
        other = lax.rem(g + off, grids)
        go(remote(field.at[other], sums.at[g], sum_send.at[off], sum_recv.at[g], b, other))
    exchange = field[g]
    for off in range(1, grids):
        other = lax.rem(g + off, grids)
        remote(phi, sums.at[other], sum_send.at[0], sum_recv.at[other], b, other).wait_recv()
        exchange = exchange + sums[other]
    exs[b] = -exchange
    for off in range(1, pairs):
        peer = lax.rem(p + off, pairs) * 2 + c
        go(remote(exs.at[b], exs.at[b], ex_send.at[off], ex_recv.at[b], peer, g))
    go(remote(exs.at[b], exs.at[b], ex_send.at[0], ex_recv.at[b], sibling, g))

    lane = lax.broadcasted_iota(jnp.int32, (8, 128), 1)
    mine = exs[b]
    total = jnp.zeros((8, 128), F32)
    for k in range(bands):
        product = jnp.sum(slabs[k] * mine, axis=0, keepdims=True)
        product = jnp.sum(product, axis=1, keepdims=True)
        total = jnp.where(lane == k, product, total)
    proj_grid[g] = total
    for off in range(1, grids):
        other = lax.rem(g + off, grids)
        go(remote(proj_grid.at[g], proj_grid.at[g], pg_send.at[off], pg_recv.at[g], b, other))
    for off in range(1, grids):
        other = lax.rem(g + off, grids)
        remote(column, proj_grid.at[other], pg_send.at[0], pg_recv.at[other], b, other).wait_recv()
    total = proj_grid[0]
    for s in range(1, grids):
        total = total + proj_grid[s]
    proj_band[b] = total
    for off in range(1, bands):
        other = lax.rem(b + off, bands)
        go(remote(proj_band.at[b], proj_band.at[b], pb_send.at[off], pb_recv.at[b], other, g))

    for off in range(1, pairs):
        band = lax.rem(p + off, pairs) * 2 + c
        remote(phi, exs.at[band], ex_send.at[0], ex_recv.at[band], sibling, g).wait_recv()
        go(remote(exs.at[band], exs.at[band], xfwd_send.at[off], ex_recv.at[band], sibling, g))

    for off in range(1, bands):
        other = lax.rem(b + off, bands)
        remote(column, proj_band.at[other], pb_send.at[0], pb_recv.at[other], other, g).wait_recv()

    row = lax.broadcasted_iota(jnp.int32, (bands, 128), 0)
    col = lax.broadcasted_iota(jnp.int32, (bands, 128), 1)
    matrix = jnp.concatenate([proj_band[l][0:1, :] for l in range(bands)], axis=0)
    mirrored = jnp.zeros((bands, 128), F32)
    for l in range(bands):
        entry = jnp.sum(jnp.where(col == l, matrix, 0.0), axis=1, keepdims=True)
        flipped = jnp.sum(jnp.where(row == col, entry, 0.0), axis=0, keepdims=True)
        mirrored = jnp.where(row == l, flipped, mirrored)
    definite = (matrix + mirrored) * (-0.5 / float(length**3))
    definite = jnp.where(col < bands, definite, jnp.where(col == row + bands, 1.0, 0.0))
    for j in range(bands):
        line = jnp.sum(jnp.where(row == j, definite, 0.0), axis=0, keepdims=True)
        entry = jnp.sum(jnp.where(col == j, definite, 0.0), axis=1, keepdims=True)
        pivot = jnp.sum(jnp.where(col[0:1] == j, line, 0.0), axis=1, keepdims=True)
        definite = definite - jnp.where(row > j, (entry / pivot) * line, 0.0)
    pick = jnp.sum(jnp.where(row == b, definite, 0.0), axis=0, keepdims=True)
    pivot = jnp.sum(jnp.where(col[0:1] == b, pick, 0.0), axis=1, keepdims=True)
    pick = pick / jnp.sqrt(pivot)

    for off in range(pairs):
        band = lax.rem(p + off, pairs) * 2 + (1 - c)
        remote(phi, exs.at[band], ex_send.at[0], ex_recv.at[band], sibling, g).wait_recv()
    result = jnp.zeros_like(mine)
    for l in range(bands):
        weight = jnp.sum(jnp.where(col[0:1] == bands + l, pick, 0.0), axis=1, keepdims=True)
        result = result + weight * exs[l]
    out[...] = result

    for copy in waits:
        copy.wait_send()
    for off in range(pairs):
        pair = lax.rem(p + off, pairs)
        copy = remote(slabs.at[pair * 2 + c], part.at[c, g], part_send.at[pair], part_recv.at[g], b, pair)

        @pl.when(pair != g)
        def _(copy=copy):
            copy.wait_send()


def per_device(bands, grids, orbitals):
    blocks, rows, cells = orbitals.shape
    length = rows * grids
    assert blocks == 1 and bands == 2 * grids and length * length == cells
    basis = real_basis(length)
    parts = []
    for table in (basis, basis.T):
        high = table.astype(np.float32).astype(BF16)
        parts += [high, (table - high.astype(np.float64)).astype(np.float32).astype(BF16)]
    tables = jnp.asarray(np.stack(parts))
    slab = (rows, cells)
    dma = lambda n: pltpu.SemaphoreType.DMA((n,))
    vmem = lambda *shape: pltpu.VMEM(shape, F32)
    pairs = bands // 2
    result = pl.pallas_call(
        functools.partial(kernel, bands, grids, length),
        out_shape=jax.ShapeDtypeStruct(slab, F32),
        in_specs=[pl.BlockSpec(memory_space=pltpu.VMEM)] * 2,
        out_specs=pl.BlockSpec(memory_space=pltpu.VMEM),
        scratch_shapes=[
            vmem(bands, *slab), vmem(grids, *slab), vmem(2, grids, *slab),
            vmem(grids, *slab), vmem(grids, *slab), vmem(bands, *slab),
            vmem(grids, 8, 128), vmem(bands, 8, 128),
            vmem(length, cells), vmem(2, length, cells),
            vmem(length, length, length), vmem(length, length, length),
            vmem(length, cells), vmem(8, 128),
            pltpu.SemaphoreType.DMA, dma(pairs), dma(bands), dma(pairs),
            dma(grids), dma(grids), dma(pairs), dma(grids), dma(grids), dma(grids),
            dma(grids), dma(grids), dma(pairs), dma(bands), dma(pairs),
            dma(grids), dma(grids), dma(bands), dma(bands),
        ],
        compiler_params=pltpu.CompilerParams(
            collective_id=0, has_side_effects=True, vmem_limit_bytes=40 * 1024 * 1024
        ),
    )(orbitals.reshape(slab), tables)
    return result.reshape(orbitals.shape)


def solution(mesh):
    bands, grids = mesh.shape["band"], mesh.shape["grid"]
    return jax.shard_map(
        functools.partial(per_device, bands, grids), mesh=mesh,
        in_specs=(P("band", "grid", None),), out_specs=P("band", "grid", None), check_vma=False,
    )
```

```python
import functools
import math

import jax
import jax.numpy as jnp
import numpy as np
from jax import lax
from jax.experimental import pallas as pl
from jax.experimental.pallas import tpu as pltpu
from jax.sharding import PartitionSpec as P

MESH = pl.DeviceIdType.MESH
F32 = jnp.float32
BF16 = jnp.bfloat16
coulomb_scale = 50.0


def real_basis(length):
    n = np.arange(length)[:, None]
    m = np.arange(length)[None, :]
    angle = 2.0 * math.pi * ((n * np.minimum(m, length - m)) % length) / length
    table = np.where(m <= length // 2, np.cos(angle), np.sin(angle))
    weight = np.where((m == 0) | (2 * m == length), 1.0, 2.0)
    return table * np.sqrt(weight / length)


def split(value):
    high = value.astype(BF16)
    return high, (value - high.astype(F32)).astype(BF16)


def times(value, high, low, contract=((1,), (0,))):
    dims = (contract, ((), ()))
    value_high, value_low = split(value)
    dot = functools.partial(lax.dot_general, dimension_numbers=dims, preferred_element_type=F32)
    return dot(value_high, high) + (dot(value_low, high) + dot(value_high, low))


def times_left(high, low, value):
    dims = (((1,), (1,)), ((), ()))
    value_high, value_low = split(value)
    dot = functools.partial(lax.dot_general, dimension_numbers=dims, preferred_element_type=F32)
    return dot(high, value_high) + (dot(high, value_low) + dot(low, value_high))


def flat(value):
    return value.reshape(value.shape[0] * value.shape[1], value.shape[2])


def kernel(
    bands, grids, length, pieces,
    phi, tables, out,
    slabs, own, part, field, sums, exs, proj_grid, proj_band,
    dense_own, dense_part, work, coulomb, dense_field,
    sem_local, slab_send, slab_recv, fwd_send,
    own_send, own_recv, part_send, part_recv, pfwd_send, pfwd_recv,
    sum_send, sum_recv, ex_send, ex_recv, xfwd_send,
    pg_send, pg_recv, pb_send, pb_recv,
):
    b = lax.axis_index("band")
    g = lax.axis_index("grid")
    p = b // 2
    c = b % 2
    sibling = p * 2 + (1 - c)
    rows = length // grids
    pairs = bands // 2
    step = 8
    chunk = step * length
    chunks = length // step
    width = length * length // pieces
    per_piece = chunks // pieces

    def remote(src, dst, send, recv, band, grid):
        return pltpu.make_async_remote_copy(
            src_ref=src, dst_ref=dst, send_sem=send, recv_sem=recv,
            device_id=(band, grid), device_id_type=MESH,
        )

    def cut(q):
        return pl.ds(q * width, width)

    local = pltpu.make_async_copy(phi, slabs.at[b], sem_local)
    local.start()

    barrier = pltpu.get_barrier_semaphore()
    for off in range(1, bands):
        pl.semaphore_signal(barrier, inc=1, device_id=(lax.rem(b + off, bands), g), device_id_type=MESH)
    for off in range(1, grids):
        pl.semaphore_signal(barrier, inc=1, device_id=(b, lax.rem(g + off, grids)), device_id_type=MESH)

    def freq(shape, dim, base):
        m = lax.broadcasted_iota(jnp.int32, shape, dim) + base
        f = jnp.minimum(m, length - m).astype(F32)
        return f * f

    def coulomb_step(i, carry):
        shape = (step, length, length)
        squared = freq(shape, 0, i * step) + freq(shape, 1, 0) + freq(shape, 2, 0)
        coulomb[pl.ds(i * step, step)] = jnp.where(
            squared > 0.0, coulomb_scale / jnp.maximum(squared, 1.0), 0.0
        )
        return carry

    lax.fori_loop(0, chunks, coulomb_step, 0)
    local.wait()
    pl.semaphore_wait(barrier, bands + grids - 2)

    waits = []

    def go(copy):
        copy.start()
        waits.append(copy)

    for q in range(pieces):
        for off in range(1, pairs):
            peer = lax.rem(p + off, pairs) * 2 + c
            go(remote(phi.at[:, cut(q)], slabs.at[b, :, cut(q)],
                      slab_send.at[off, q], slab_recv.at[b, q], peer, g))
        for off in range(1, grids):
            go(remote(phi.at[:, cut(q)], own.at[g, :, cut(q)],
                      own_send.at[off, q], own_recv.at[g, q], b, lax.rem(g + off, grids)))
        go(remote(phi.at[:, cut(q)], slabs.at[b, :, cut(q)],
                  slab_send.at[0, q], slab_recv.at[b, q], sibling, g))

    def partner_copy(pair, q):
        return remote(
            slabs.at[pair * 2 + c, :, cut(q)], part.at[c, g, :, cut(q)],
            part_send.at[pair, q], part_recv.at[g, q], b, pair,
        )

    def to_partner(pair, q):
        @pl.when(pair != g)
        def _():
            partner_copy(pair, q).start()

    def slab_arrival(band, q):
        here = slabs.at[band, :, cut(q)]
        remote(here, here, slab_send.at[0, q], slab_recv.at[band, q], sibling, g).wait_recv()

    def pass_slabs(q):
        to_partner(p, q)
        for off in range(1, pairs):
            pair = lax.rem(p + off, pairs)
            band = pair * 2 + c
            slab_arrival(band, q)
            to_partner(pair, q)
            here = slabs.at[band, :, cut(q)]
            go(remote(here, here, fwd_send.at[off, q], slab_recv.at[band, q], sibling, g))

    def pass_partners(q):
        for off in range(1, grids):
            other = lax.rem(g + off, grids)
            here = part.at[c, other, :, cut(q)]
            remote(here, here, part_send.at[0, q], part_recv.at[other, q], b, other).wait_recv()
            go(remote(here, here, pfwd_send.at[off, q], pfwd_recv.at[other, q], sibling, g))

    def collect(q):
        slab_arrival(2 * g + 1 - c, q)
        for off in range(1, grids):
            other = lax.rem(g + off, grids)
            here = own.at[other, :, cut(q)]
            remote(here, here, own_send.at[0, q], own_recv.at[other, q], b, other).wait_recv()
            here = part.at[1 - c, other, :, cut(q)]
            remote(here, here, part_send.at[0, q], pfwd_recv.at[other, q], sibling, g).wait_recv()
        own[g, :, cut(q)] = phi[:, cut(q)]
        for k in range(2):
            part[k, g, :, cut(q)] = slabs[2 * g + k, :, cut(q)]
        for s in range(grids):
            here = slice(s * rows, (s + 1) * rows)
            dense_own[here, cut(q)] = own[s, :, cut(q)]
            for k in range(2):
                dense_part[k, here, cut(q)] = part[k, s, :, cut(q)]

    q_high, q_low, t_high, t_low = (tables[n] for n in range(4))

    def swap(value):
        return jnp.swapaxes(value, 1, 2)

    def unflat(value):
        return value.reshape(value.shape[0] // length, length, length)

    def lanes_of(i):
        return pl.ds(pl.multiple_of(i * chunk, 128), chunk)

    def stage_in(i, carry):
        lanes = lanes_of(i)
        for k in range(2):
            density = dense_own[:, lanes] * dense_part[k, :, lanes]
            first = unflat(times(density.T, q_high, q_low))
            work[k, pl.ds(i * step, step)] = unflat(times(flat(swap(first)), q_high, q_low))
        return carry

    def stage_mid(i, carry):
        here = pl.ds(pl.multiple_of(i * step, step), step)
        for k in range(2):
            value = jnp.swapaxes(work[k, :, here, :], 0, 1)
            value = unflat(times(flat(swap(value)), q_high, q_low))
            value = value * coulomb[pl.ds(i * step, step)]
            value = unflat(times(flat(value), t_high, t_low))
            work[k, :, here, :] = jnp.swapaxes(swap(value), 0, 1)
        return carry

    def send_sums(i):
        lanes = lanes_of(i)
        for off in range(1, grids):
            other = lax.rem(g + off, grids)
            remote(field.at[other, :, lanes], sums.at[g, :, lanes],
                   sum_send.at[off, i], sum_recv.at[g, i], b, other).start()

    def stage_out(i, carry):
        lanes = lanes_of(i)
        term = None
        for k in range(2):
            value = unflat(times(flat(work[k, pl.ds(i * step, step)]), t_high, t_low))
            here = dense_part[k, :, lanes] * times_left(q_high, q_low, flat(swap(value)))
            term = here if term is None else term + here
        dense_field[...] = term
        for s in range(grids):
            field[s, :, lanes] = dense_field[s * rows:(s + 1) * rows, :]

        @pl.when(i > 0)
        def _():
            send_sums(i - 1)

        return carry

    columns = [None] * bands

    def exchange_piece(q):
        for i in range(q * per_piece, (q + 1) * per_piece):
            lanes = pl.ds(i * chunk, chunk)
            for off in range(1, grids):
                other = lax.rem(g + off, grids)
                here = sums.at[other, :, lanes]
                remote(here, here, sum_send.at[0, i], sum_recv.at[other, i], b, other).wait_recv()
        value = field[g, :, cut(q)]
        for off in range(1, grids):
            value = value + sums[lax.rem(g + off, grids), :, cut(q)]
        value = -value
        exs[b, :, cut(q)] = value
        for k in range(bands):
            product = jnp.sum(slabs[k, :, cut(q)] * value, axis=0, keepdims=True)
            product = sum(product[:, n:n + 128] for n in range(0, width, 128))
            columns[k] = product if columns[k] is None else columns[k] + product
        here = exs.at[b, :, cut(q)]
        for off in range(1, pairs):
            peer = lax.rem(p + off, pairs) * 2 + c
            go(remote(here, here, ex_send.at[off, q], ex_recv.at[b, q], peer, g))
        go(remote(here, here, ex_send.at[0, q], ex_recv.at[b, q], sibling, g))

    for q in range(pieces):
        pass_slabs(q)
        if q >= 1:
            pass_partners(q - 1)
    for q in range(pieces):
        collect(q)
        lax.fori_loop(q * per_piece, (q + 1) * per_piece, stage_in, 0)
        if q == 0:
            pass_partners(pieces - 1)
    lax.fori_loop(0, chunks, stage_mid, 0)
    for q in range(pieces):
        for off in range(pairs):
            pair = lax.rem(p + off, pairs)

            @pl.when(pair != g)
            def _(pair=pair, q=q):
                slab_arrival(pair * 2 + 1 - c, q)

    for q in range(pieces):
        lax.fori_loop(q * per_piece, (q + 1) * per_piece, stage_out, 0)
        if q >= 1:
            exchange_piece(q - 1)
    send_sums(chunks - 1)
    exchange_piece(pieces - 1)

    total = jnp.sum(jnp.concatenate(columns, axis=0), axis=1, keepdims=True)
    proj_grid[g] = jnp.broadcast_to(total, (bands, 128))
    for off in range(1, grids):
        other = lax.rem(g + off, grids)
        go(remote(proj_grid.at[g], proj_grid.at[g], pg_send.at[off], pg_recv.at[g], b, other))

    def ex_arrival(band, q):
        here = exs.at[band, :, cut(q)]
        remote(here, here, ex_send.at[0, q], ex_recv.at[band, q], sibling, g).wait_recv()

    def pass_exchange(q):
        for off in range(1, pairs):
            band = lax.rem(p + off, pairs) * 2 + c
            ex_arrival(band, q)
            here = exs.at[band, :, cut(q)]
            go(remote(here, here, xfwd_send.at[off, q], ex_recv.at[band, q], sibling, g))

    pass_exchange(0)
    for off in range(1, grids):
        other = lax.rem(g + off, grids)
        here = proj_grid.at[other]
        remote(here, here, pg_send.at[0], pg_recv.at[other], b, other).wait_recv()
    total = proj_grid[0]
    for s in range(1, grids):
        total = total + proj_grid[s]
    proj_band[b] = total
    for off in range(1, bands):
        other = lax.rem(b + off, bands)
        go(remote(proj_band.at[b], proj_band.at[b], pb_send.at[off], pb_recv.at[b], other, g))
    for q in range(1, pieces):
        pass_exchange(q)
    for off in range(1, bands):
        other = lax.rem(b + off, bands)
        here = proj_band.at[other]
        remote(here, here, pb_send.at[0], pb_recv.at[other], other, g).wait_recv()

    row = lax.broadcasted_iota(jnp.int32, (bands, 128), 0)
    col = lax.broadcasted_iota(jnp.int32, (bands, 128), 1)
    matrix = jnp.zeros((bands, 128), F32)
    mirrored = jnp.zeros((bands, 128), F32)
    for l in range(bands):
        entries = proj_band[l]
        matrix = jnp.where(col == l, entries, matrix)
        flipped = jnp.sum(jnp.where(row == col, entries, 0.0), axis=0, keepdims=True)
        mirrored = jnp.where(row == l, flipped, mirrored)
    definite = (matrix + mirrored) * (-0.5 / float(length**3))
    definite = jnp.where(col < bands, definite, jnp.where(col == row + bands, 1.0, 0.0))
    for j in range(bands - 1):
        line = definite[j:j + 1, :]
        ratio = definite[:, j:j + 1] / definite[j:j + 1, j:j + 1]
        definite = definite - jnp.where(row > j, ratio * line, 0.0)
    pick = jnp.sum(jnp.where(row == b, definite, 0.0), axis=0, keepdims=True)
    pivot = jnp.sum(jnp.where(col[0:1] == b, pick, 0.0), axis=1, keepdims=True)
    pick = pick / jnp.sqrt(pivot)

    for q in range(pieces):
        for off in range(pairs):
            ex_arrival(lax.rem(p + off, pairs) * 2 + (1 - c), q)
    result = jnp.zeros(phi.shape, F32)
    for l in range(bands):
        result = result + pick[:, bands + l:bands + l + 1] * exs[l]
    out[...] = result

    for copy in waits:
        copy.wait_send()
    for i in range(chunks):
        lanes = pl.ds(i * chunk, chunk)
        for off in range(1, grids):
            other = lax.rem(g + off, grids)
            remote(field.at[other, :, lanes], sums.at[g, :, lanes],
                   sum_send.at[off, i], sum_recv.at[g, i], b, other).wait_send()
    for q in range(pieces):
        for off in range(pairs):
            pair = lax.rem(p + off, pairs)

            @pl.when(pair != g)
            def _(pair=pair, q=q):
                partner_copy(pair, q).wait_send()


def per_device(bands, grids, orbitals):
    blocks, rows, cells = orbitals.shape
    length = rows * grids
    assert blocks == 1 and bands == 2 * grids and length * length == cells
    basis = real_basis(length)
    parts = []
    for table in (basis, basis.T):
        high = table.astype(np.float32).astype(BF16)
        parts += [high, (table - high.astype(np.float64)).astype(np.float32).astype(BF16)]
    tables = jnp.asarray(np.stack(parts))
    slab = (rows, cells)
    dma = lambda *n: pltpu.SemaphoreType.DMA(n)
    vmem = lambda *shape: pltpu.VMEM(shape, F32)
    pairs = bands // 2
    pieces = 3
    chunks = length // 8
    result = pl.pallas_call(
        functools.partial(kernel, bands, grids, length, pieces),
        out_shape=jax.ShapeDtypeStruct(slab, F32),
        in_specs=[pl.BlockSpec(memory_space=pltpu.VMEM)] * 2,
        out_specs=pl.BlockSpec(memory_space=pltpu.VMEM),
        scratch_shapes=[
            vmem(bands, *slab), vmem(grids, *slab), vmem(2, grids, *slab),
            vmem(grids, *slab), vmem(grids, *slab), vmem(bands, *slab),
            vmem(grids, bands, 128), vmem(bands, bands, 128),
            vmem(length, cells), vmem(2, length, cells),
            vmem(2, length, length, length), vmem(length, length, length),
            vmem(length, 8 * length),
            pltpu.SemaphoreType.DMA,
            dma(pairs, pieces), dma(bands, pieces), dma(pairs, pieces),
            dma(grids, pieces), dma(grids, pieces), dma(pairs, pieces), dma(grids, pieces),
            dma(grids, pieces), dma(grids, pieces),
            dma(grids, chunks), dma(grids, chunks),
            dma(pairs, pieces), dma(bands, pieces), dma(pairs, pieces),
            dma(grids), dma(grids), dma(bands), dma(bands),
        ],
        compiler_params=pltpu.CompilerParams(
            collective_id=0, has_side_effects=True, vmem_limit_bytes=40 * 1024 * 1024
        ),
    )(orbitals.reshape(slab), tables)
    return result.reshape(orbitals.shape)


def solution(mesh):
    bands, grids = mesh.shape["band"], mesh.shape["grid"]
    return jax.shard_map(
        functools.partial(per_device, bands, grids), mesh=mesh,
        in_specs=(P("band", "grid", None),), out_specs=P("band", "grid", None), check_vma=False,
    )
```

```python
import functools
import math

import jax
import jax.numpy as jnp
import numpy as np
from jax import lax
from jax.experimental import pallas as pl
from jax.experimental.pallas import tpu as pltpu
from jax.sharding import PartitionSpec as P

MESH = pl.DeviceIdType.MESH
F32 = jnp.float32
BF16 = jnp.bfloat16
coulomb_scale = 50.0


def real_basis(length):
    n = np.arange(length)[:, None]
    m = np.arange(length)[None, :]
    angle = 2.0 * math.pi * ((n * np.minimum(m, length - m)) % length) / length
    table = np.where(m <= length // 2, np.cos(angle), np.sin(angle))
    weight = np.where((m == 0) | (2 * m == length), 1.0, 2.0)
    return table * np.sqrt(weight / length)


def split(value):
    high = value.astype(BF16)
    return high, (value - high.astype(F32)).astype(BF16)


def times(value, high, low, contract=((1,), (0,))):
    dims = (contract, ((), ()))
    value_high, value_low = split(value)
    dot = functools.partial(lax.dot_general, dimension_numbers=dims, preferred_element_type=F32)
    return dot(value_high, high) + (dot(value_low, high) + dot(value_high, low))


def times_left(high, low, value):
    dims = (((1,), (1,)), ((), ()))
    value_high, value_low = split(value)
    dot = functools.partial(lax.dot_general, dimension_numbers=dims, preferred_element_type=F32)
    return dot(high, value_high) + (dot(high, value_low) + dot(low, value_high))


def flat(value):
    return value.reshape(value.shape[0] * value.shape[1], value.shape[2])


def kernel(
    bands, grids, length, pieces,
    phi, tables, out,
    slabs, own, part, field, sums, exs, proj_grid, proj_band,
    dense_own, dense_part, work, coulomb, dense_field,
    sem_local, slab_send, slab_recv, fwd_send,
    own_send, own_recv, part_send, part_recv, pfwd_send, pfwd_recv,
    sum_send, sum_recv, ex_send, ex_recv, xfwd_send,
    pg_send, pg_recv, pb_send, pb_recv,
):
    b = lax.axis_index("band")
    g = lax.axis_index("grid")
    p = b // 2
    c = b % 2
    sibling = p * 2 + (1 - c)
    rows = length // grids
    pairs = bands // 2
    step = 8
    chunk = step * length
    chunks = length // step
    width = length * length // pieces
    per_piece = chunks // pieces

    def remote(src, dst, send, recv, band, grid):
        return pltpu.make_async_remote_copy(
            src_ref=src, dst_ref=dst, send_sem=send, recv_sem=recv,
            device_id=(band, grid), device_id_type=MESH,
        )

    def cut(q):
        return pl.ds(q * width, width)

    local = pltpu.make_async_copy(phi, slabs.at[b], sem_local)
    local.start()

    barrier = pltpu.get_barrier_semaphore()
    for off in range(1, bands):
        pl.semaphore_signal(barrier, inc=1, device_id=(lax.rem(b + off, bands), g), device_id_type=MESH)
    for off in range(1, grids):
        pl.semaphore_signal(barrier, inc=1, device_id=(b, lax.rem(g + off, grids)), device_id_type=MESH)

    def freq(shape, dim, base):
        m = lax.broadcasted_iota(jnp.int32, shape, dim) + base
        f = jnp.minimum(m, length - m).astype(F32)
        return f * f

    def coulomb_step(i, carry):
        shape = (step, length, length)
        squared = freq(shape, 0, i * step) + freq(shape, 1, 0) + freq(shape, 2, 0)
        coulomb[pl.ds(i * step, step)] = jnp.where(
            squared > 0.0, coulomb_scale / jnp.maximum(squared, 1.0), 0.0
        )
        return carry

    lax.fori_loop(0, chunks, coulomb_step, 0)
    local.wait()
    pl.semaphore_wait(barrier, bands + grids - 2)

    waits = []

    def go(copy):
        copy.start()
        waits.append(copy)

    for q in range(pieces):
        for off in range(1, pairs):
            peer = lax.rem(p + off, pairs) * 2 + c
            go(remote(phi.at[:, cut(q)], slabs.at[b, :, cut(q)],
                      slab_send.at[off, q], slab_recv.at[b, q], peer, g))
        for off in range(1, grids):
            go(remote(phi.at[:, cut(q)], own.at[g, :, cut(q)],
                      own_send.at[off, q], own_recv.at[g, q], b, lax.rem(g + off, grids)))
        go(remote(phi.at[:, cut(q)], slabs.at[b, :, cut(q)],
                  slab_send.at[0, q], slab_recv.at[b, q], sibling, g))

    def partner_copy(pair, q):
        return remote(
            slabs.at[pair * 2 + c, :, cut(q)], part.at[c, g, :, cut(q)],
            part_send.at[pair, q], part_recv.at[g, q], b, pair,
        )

    def to_partner(pair, q):
        @pl.when(pair != g)
        def _():
            partner_copy(pair, q).start()

    def slab_arrival(band, q):
        here = slabs.at[band, :, cut(q)]
        remote(here, here, slab_send.at[0, q], slab_recv.at[band, q], sibling, g).wait_recv()

    def pass_slabs(q):
        to_partner(p, q)
        for off in range(1, pairs):
            pair = lax.rem(p + off, pairs)
            band = pair * 2 + c
            slab_arrival(band, q)
            to_partner(pair, q)
            here = slabs.at[band, :, cut(q)]
            go(remote(here, here, fwd_send.at[off, q], slab_recv.at[band, q], sibling, g))

    def pass_partners(q):
        for off in range(1, grids):
            other = lax.rem(g + off, grids)
            here = part.at[c, other, :, cut(q)]
            remote(here, here, part_send.at[0, q], part_recv.at[other, q], b, other).wait_recv()
            go(remote(here, here, pfwd_send.at[off, q], pfwd_recv.at[other, q], sibling, g))

    def collect(q):
        slab_arrival(2 * g + 1 - c, q)
        for off in range(1, grids):
            other = lax.rem(g + off, grids)
            here = own.at[other, :, cut(q)]
            remote(here, here, own_send.at[0, q], own_recv.at[other, q], b, other).wait_recv()
            here = part.at[1 - c, other, :, cut(q)]
            remote(here, here, part_send.at[0, q], pfwd_recv.at[other, q], sibling, g).wait_recv()
        own[g, :, cut(q)] = phi[:, cut(q)]
        for k in range(2):
            part[k, g, :, cut(q)] = slabs[2 * g + k, :, cut(q)]
        for s in range(grids):
            here = slice(s * rows, (s + 1) * rows)
            dense_own[here, cut(q)] = own[s, :, cut(q)]
            for k in range(2):
                dense_part[k, here, cut(q)] = part[k, s, :, cut(q)]

    q_high, q_low, t_high, t_low = (tables[n] for n in range(4))

    def swap(value):
        return jnp.swapaxes(value, 1, 2)

    def unflat(value):
        return value.reshape(value.shape[0] // length, length, length)

    def lanes_of(i):
        return pl.ds(pl.multiple_of(i * chunk, 128), chunk)

    def stage_in(i, carry):
        lanes = lanes_of(i)
        for k in range(2):
            density = dense_own[:, lanes] * dense_part[k, :, lanes]
            first = unflat(times(density.T, q_high, q_low))
            work[k, pl.ds(i * step, step)] = unflat(times(flat(swap(first)), q_high, q_low))
        return carry

    def stage_mid(i, carry):
        here = pl.ds(pl.multiple_of(i * step, step), step)
        for k in range(2):
            value = jnp.swapaxes(work[k, :, here, :], 0, 1)
            value = unflat(times(flat(swap(value)), q_high, q_low))
            value = value * coulomb[pl.ds(i * step, step)]
            value = unflat(times(flat(value), t_high, t_low))
            work[k, :, here, :] = jnp.swapaxes(swap(value), 0, 1)
        return carry

    def send_sums(i):
        lanes = lanes_of(i)
        for off in range(1, grids):
            other = lax.rem(g + off, grids)
            remote(field.at[other, :, lanes], sums.at[g, :, lanes],
                   sum_send.at[off, i], sum_recv.at[g, i], b, other).start()

    def stage_out(i, carry):
        lanes = lanes_of(i)
        term = None
        for k in range(2):
            value = unflat(times(flat(work[k, pl.ds(i * step, step)]), t_high, t_low))
            here = dense_part[k, :, lanes] * times_left(q_high, q_low, flat(swap(value)))
            term = here if term is None else term + here
        dense_field[...] = term
        for s in range(grids):
            field[s, :, lanes] = dense_field[s * rows:(s + 1) * rows, :]

        @pl.when(i > 0)
        def _():
            send_sums(i - 1)

        return carry

    columns = [None] * bands

    def exchange_piece(q):
        for i in range(q * per_piece, (q + 1) * per_piece):
            lanes = pl.ds(i * chunk, chunk)
            for off in range(1, grids):
                other = lax.rem(g + off, grids)
                here = sums.at[other, :, lanes]
                remote(here, here, sum_send.at[0, i], sum_recv.at[other, i], b, other).wait_recv()
        value = field[g, :, cut(q)]
        for off in range(1, grids):
            value = value + sums[lax.rem(g + off, grids), :, cut(q)]
        value = -value
        exs[b, :, cut(q)] = value
        for k in range(bands):
            product = jnp.sum(slabs[k, :, cut(q)] * value, axis=0, keepdims=True)
            product = sum(product[:, n:n + 128] for n in range(0, width, 128))
            columns[k] = product if columns[k] is None else columns[k] + product
        here = exs.at[b, :, cut(q)]
        for off in range(1, pairs):
            peer = lax.rem(p + off, pairs) * 2 + c
            go(remote(here, here, ex_send.at[off, q], ex_recv.at[b, q], peer, g))
        go(remote(here, here, ex_send.at[0, q], ex_recv.at[b, q], sibling, g))

    for q in range(pieces):
        pass_slabs(q)
        if q >= 1:
            pass_partners(q - 1)
    for q in range(pieces):
        collect(q)
        lax.fori_loop(q * per_piece, (q + 1) * per_piece, stage_in, 0)
        if q == 0:
            pass_partners(pieces - 1)
    lax.fori_loop(0, chunks, stage_mid, 0)
    for q in range(pieces):
        for off in range(pairs):
            pair = lax.rem(p + off, pairs)

            @pl.when(pair != g)
            def _(pair=pair, q=q):
                slab_arrival(pair * 2 + 1 - c, q)

    for q in range(pieces):
        lax.fori_loop(q * per_piece, (q + 1) * per_piece, stage_out, 0)
    send_sums(chunks - 1)
    for q in range(pieces):
        exchange_piece(q)

    total = jnp.sum(jnp.concatenate(columns, axis=0), axis=1, keepdims=True)
    proj_grid[g] = jnp.broadcast_to(total, (bands, 128))
    for off in range(1, grids):
        other = lax.rem(g + off, grids)
        go(remote(proj_grid.at[g], proj_grid.at[g], pg_send.at[off], pg_recv.at[g], b, other))

    def ex_arrival(band, q):
        here = exs.at[band, :, cut(q)]
        remote(here, here, ex_send.at[0, q], ex_recv.at[band, q], sibling, g).wait_recv()

    def pass_exchange(q):
        for off in range(1, pairs):
            band = lax.rem(p + off, pairs) * 2 + c
            ex_arrival(band, q)
            here = exs.at[band, :, cut(q)]
            go(remote(here, here, xfwd_send.at[off, q], ex_recv.at[band, q], sibling, g))

    pass_exchange(0)
    for off in range(1, grids):
        other = lax.rem(g + off, grids)
        here = proj_grid.at[other]
        remote(here, here, pg_send.at[0], pg_recv.at[other], b, other).wait_recv()
    total = proj_grid[0]
    for s in range(1, grids):
        total = total + proj_grid[s]
    proj_band[b] = total
    for off in range(1, bands):
        other = lax.rem(b + off, bands)
        go(remote(proj_band.at[b], proj_band.at[b], pb_send.at[off], pb_recv.at[b], other, g))
    for q in range(1, pieces):
        pass_exchange(q)
    for off in range(1, bands):
        other = lax.rem(b + off, bands)
        here = proj_band.at[other]
        remote(here, here, pb_send.at[0], pb_recv.at[other], other, g).wait_recv()

    row = lax.broadcasted_iota(jnp.int32, (bands, 128), 0)
    col = lax.broadcasted_iota(jnp.int32, (bands, 128), 1)
    matrix = jnp.zeros((bands, 128), F32)
    mirrored = jnp.zeros((bands, 128), F32)
    for l in range(bands):
        entries = proj_band[l]
        matrix = jnp.where(col == l, entries, matrix)
        flipped = jnp.sum(jnp.where(row == col, entries, 0.0), axis=0, keepdims=True)
        mirrored = jnp.where(row == l, flipped, mirrored)
    definite = (matrix + mirrored) * (-0.5 / float(length**3))
    definite = jnp.where(col < bands, definite, jnp.where(col == row + bands, 1.0, 0.0))
    for j in range(bands - 1):
        line = definite[j:j + 1, :]
        ratio = definite[:, j:j + 1] / definite[j:j + 1, j:j + 1]
        definite = definite - jnp.where(row > j, ratio * line, 0.0)
    pick = jnp.sum(jnp.where(row == b, definite, 0.0), axis=0, keepdims=True)
    pivot = jnp.sum(jnp.where(col[0:1] == b, pick, 0.0), axis=1, keepdims=True)
    pick = pick / jnp.sqrt(pivot)

    for q in range(pieces):
        for off in range(pairs):
            ex_arrival(lax.rem(p + off, pairs) * 2 + (1 - c), q)
    result = jnp.zeros(phi.shape, F32)
    for l in range(bands):
        result = result + pick[:, bands + l:bands + l + 1] * exs[l]
    out[...] = result

    for copy in waits:
        copy.wait_send()
    for i in range(chunks):
        lanes = pl.ds(i * chunk, chunk)
        for off in range(1, grids):
            other = lax.rem(g + off, grids)
            remote(field.at[other, :, lanes], sums.at[g, :, lanes],
                   sum_send.at[off, i], sum_recv.at[g, i], b, other).wait_send()
    for q in range(pieces):
        for off in range(pairs):
            pair = lax.rem(p + off, pairs)

            @pl.when(pair != g)
            def _(pair=pair, q=q):
                partner_copy(pair, q).wait_send()


def per_device(bands, grids, orbitals):
    blocks, rows, cells = orbitals.shape
    length = rows * grids
    assert blocks == 1 and bands == 2 * grids and length * length == cells
    basis = real_basis(length)
    parts = []
    for table in (basis, basis.T):
        high = table.astype(np.float32).astype(BF16)
        parts += [high, (table - high.astype(np.float64)).astype(np.float32).astype(BF16)]
    tables = jnp.asarray(np.stack(parts))
    slab = (rows, cells)
    dma = lambda *n: pltpu.SemaphoreType.DMA(n)
    vmem = lambda *shape: pltpu.VMEM(shape, F32)
    pairs = bands // 2
    pieces = 3
    chunks = length // 8
    result = pl.pallas_call(
        functools.partial(kernel, bands, grids, length, pieces),
        out_shape=jax.ShapeDtypeStruct(slab, F32),
        in_specs=[pl.BlockSpec(memory_space=pltpu.VMEM)] * 2,
        out_specs=pl.BlockSpec(memory_space=pltpu.VMEM),
        scratch_shapes=[
            vmem(bands, *slab), vmem(grids, *slab), vmem(2, grids, *slab),
            vmem(grids, *slab), vmem(grids, *slab), vmem(bands, *slab),
            vmem(grids, bands, 128), vmem(bands, bands, 128),
            vmem(length, cells), vmem(2, length, cells),
            vmem(2, length, length, length), vmem(length, length, length),
            vmem(length, 8 * length),
            pltpu.SemaphoreType.DMA,
            dma(pairs, pieces), dma(bands, pieces), dma(pairs, pieces),
            dma(grids, pieces), dma(grids, pieces), dma(pairs, pieces), dma(grids, pieces),
            dma(grids, pieces), dma(grids, pieces),
            dma(grids, chunks), dma(grids, chunks),
            dma(pairs, pieces), dma(bands, pieces), dma(pairs, pieces),
            dma(grids), dma(grids), dma(bands), dma(bands),
        ],
        compiler_params=pltpu.CompilerParams(
            collective_id=0, has_side_effects=True, vmem_limit_bytes=40 * 1024 * 1024
        ),
    )(orbitals.reshape(slab), tables)
    return result.reshape(orbitals.shape)


def solution(mesh):
    bands, grids = mesh.shape["band"], mesh.shape["grid"]
    return jax.shard_map(
        functools.partial(per_device, bands, grids), mesh=mesh,
        in_specs=(P("band", "grid", None),), out_specs=P("band", "grid", None), check_vma=False,
    )
```
